32 devices in a mesh: groups: 2 (over x), dp: 2 (over core), seq: 8 (over z, y).
Axes of the slice: x: 2, y: 2, z: 4, core: 2. Of those that a mesh axis runs over, the one named last changes fastest.
Arguments:
- history: bfloat16 [8, 768, 1024], P(('groups', 'dp'), 'seq'), parts along dimension 0, may hold values from -20 to 20
- candidates: bfloat16 [4, 512, 1024], P(('groups', 'dp'), 'seq'), parts along dimension 0, may hold values from -6 to 6
- lengths: int32 [8], P(('groups', 'dp')), parts along dimension 0, may hold values from 96 to 768
- assignment: int32 [4, 512], P(('groups', 'dp'), 'seq'), parts along dimension 0, may hold values from 0 to 1, as said below
- weight_in: bfloat16 [1024, 4096], replicated, may hold values from -0.1875 to 0.1875
- weight_out: bfloat16 [1024, 1024], replicated, may hold values from -0.1875 to 0.1875
- gain_in: float32 [1024], replicated, may hold values from 0.25 to 1.75
- gain_attn: float32 [1024], replicated, may hold values from 0.25 to 1.75
Outputs:
- history_out: bfloat16 [8, 768, 1024], P(('groups', 'dp'), 'seq'), parts along dimension 0
- candidate_out: bfloat16 [4, 512, 1024], P(('groups', 'dp'), 'seq'), parts along dimension 0
The draws below stay inside these ranges and needn't reach their ends.
There are 2 independent parts, one for each index of `groups`. The reference program is written for one: setup_inputs(seed, part) draws one part's arguments, and reference() takes and returns one part's arrays. A program takes and returns all parts, laid end to end along the dimension named above; an argument that names none is the same for every part. Nothing has to cross between parts.
Inputs may be any that keep to these rules, and one draw needn't show every extreme that they name: `assignment`: of the 64 candidates of one device, at most 40 belong to either history; in every dp index some device has exactly 40 of the first and another exactly 40 of the second.
All inputs are finite; a program needn't handle non-finite values.
Results may differ from the reference program's by a relative error of at most 0.0075.
Values may be sent and summed in bfloat16 or wider, within the bound.
A program may use at most 192 MiB of HBM per device.

```python
import math
import jax
import jax.numpy as jnp
from jax import lax

D = 1024
H = 16
HD = 64
HIST_DP = 2
CAND_DEV = 64
LENGTH = 768
CAP = 40
HISTS = 4
CS = 512
N_DP = 2
N_SEQ = 8


def draw_history(key, part):
    first_key = jax.random.fold_in(key, 11)
    base = jnp.clip(jax.random.normal(first_key, (HISTS, LENGTH, D), jnp.float32), -4.0, 4.0)
    return base.astype(jnp.bfloat16)


def draw_assignment(key, part):
    count_key = jax.random.fold_in(key, 21)
    full_key = jax.random.fold_in(key, 22)
    other_key = jax.random.fold_in(key, 23)
    order_key = jax.random.fold_in(key, 24)
    counts = jax.random.randint(count_key, (N_DP, N_SEQ), CAND_DEV - CAP, CAP + 1)
    full_block = jax.random.randint(full_key, (N_DP, 1), 0, N_SEQ)
    other_block = (full_block + 1 + jax.random.randint(other_key, (N_DP, 1), 0, N_SEQ - 1)) % N_SEQ
    blocks = jnp.arange(N_SEQ, dtype=jnp.int32)[None, :]
    counts = jnp.where(blocks == full_block, CAP, counts)
    counts = jnp.where(blocks == other_block, CAND_DEV - CAP, counts)
    row_keys = jax.random.split(order_key, N_DP * N_SEQ)
    ranks = jax.vmap(lambda one_key: jax.random.permutation(one_key, jnp.arange(CAND_DEV, dtype=jnp.int32)))(row_keys)
    ranks = ranks.reshape(N_DP, N_SEQ, CAND_DEV)
    chosen = (ranks >= counts[:, :, None]).astype(jnp.int32)
    return chosen.reshape(N_DP, CS)


def touch_ends(array, own_key, low, top_value):
    place = [jax.random.randint(jax.random.fold_in(own_key, axis), (), 0, length) for axis, length in enumerate(array.shape)]
    main_axis = array.shape.index(max(array.shape))
    neighbour = place[:main_axis] + [(place[main_axis] + 1) % array.shape[main_axis]] + place[main_axis + 1:]
    return array.at[tuple(place)].set(low).at[tuple(neighbour)].set(top_value)


def block_levels(rng, dims, pieces, low, largest):
    level = 1.0
    for dim, blocks in pieces:
        heights = jax.random.uniform(jax.random.fold_in(jax.random.fold_in(rng, 6), dim), (blocks,), jnp.float32, low / len(pieces), largest / len(pieces))
        level = level * jnp.repeat(jnp.exp(heights), dims[dim] // blocks).reshape((-1,) + (1,) * (len(dims) - 1 - dim))
    return level


def normal_values(own_key, dims, width, limit, cuts=(), kind=jnp.bfloat16):
    entries = jax.random.normal(own_key, dims, jnp.float32) * width
    if len(cuts) > 0:
        entries = block_levels(own_key, dims, cuts, -0.22, 0.18) * entries
    return jnp.clip(entries, min=-limit, max=limit).astype(kind)


def setup_inputs(seed: int = 0, part: int = 0) -> dict:
    seeds = jax.random.split(jax.random.key(seed), 9)
    part_splits = jax.random.split(jax.random.fold_in(seeds[8], part), 9)
    history = draw_history(jax.random.fold_in(jax.random.fold_in(seeds[8], part), 71), part)
    candidates = normal_values(part_splits[1], (N_DP, CS, D), 1.0, 6.0, ((0, 2), (1, 8)))
    lengths = touch_ends(jax.random.randint(part_splits[2], (HISTS,), LENGTH // 8, LENGTH + 1), jax.random.fold_in(part_splits[2], 1), LENGTH // 8, LENGTH).astype(jnp.int32)
    assignment = draw_assignment(jax.random.fold_in(jax.random.fold_in(seeds[8], part), 71), part)
    weight_in = normal_values(seeds[4], (D, 4 * D), D ** -0.5, 0.1875)
    weight_out = normal_values(seeds[5], (D, D), D ** -0.5, 0.1875)
    gain_in = jnp.clip(1.0 + 0.15 * jax.random.normal(seeds[6], (D,), jnp.float32), 0.25, 1.75)
    gain_attn = jnp.clip(1.0 + 0.15 * jax.random.normal(seeds[7], (D,), jnp.float32), 0.25, 1.75)
    return {"history": history, "candidates": candidates, "lengths": lengths, "assignment": assignment, "weight_in": weight_in, "weight_out": weight_out, "gain_in": gain_in, "gain_attn": gain_attn}


def rms_apply(values, gain):
    return values * lax.rsqrt(lax.optimization_barrier(jnp.mean(values * values, axis=-1, keepdims=True)) + 1e-06) * gain

def self_history(packed):
    query, keys, values, valid = packed
    score_scale = HD ** (-0.5)
    scores = jnp.einsum('ihe,jhe->hij', query.astype(jnp.float32), keys.astype(jnp.float32)) * score_scale
    positions = jnp.arange(LENGTH, dtype=jnp.int32)
    allowed = (positions[None, :] <= positions[:, None]) & (positions[None, :] < valid)
    weights = jnp.where(allowed[None], jax.nn.silu(scores), 0.0).astype(jnp.bfloat16)
    result = jnp.einsum('hij,jhe->ihe', weights.astype(jnp.float32), values.astype(jnp.float32))
    return result.astype(jnp.bfloat16).reshape(LENGTH, D)

def reference(history, candidates, lengths, assignment, weight_in, weight_out, gain_in, gain_attn):
    score_scale = HD ** (-0.5)
    hist_float = history.astype(jnp.float32)
    normed = rms_apply(hist_float, gain_in).astype(jnp.bfloat16).reshape(HISTS * LENGTH, D)
    projected = jnp.dot(normed, weight_in, preferred_element_type=jnp.float32)
    gate = jax.nn.silu(projected[:, :D]).astype(jnp.bfloat16)
    query = projected[:, D:2 * D].astype(jnp.bfloat16).reshape(HISTS, LENGTH, H, HD)
    keys = projected[:, 2 * D:3 * D].astype(jnp.bfloat16).reshape(HISTS, LENGTH, H, HD)
    values = projected[:, 3 * D:].astype(jnp.bfloat16).reshape(HISTS, LENGTH, H, HD)
    attended = lax.map(self_history, (query, keys, values, lengths))
    attended = attended.reshape(HISTS * LENGTH, D).astype(jnp.float32)
    gated_rows = (rms_apply(attended, gain_attn) * gate.astype(jnp.float32)).astype(jnp.bfloat16)
    history_out = (hist_float.reshape(HISTS * LENGTH, D) + jnp.dot(gated_rows, weight_out, preferred_element_type=jnp.float32)).astype(jnp.bfloat16)
    history_out = history_out.reshape(HISTS, LENGTH, D)
    cand_float = candidates.astype(jnp.float32)
    cand_normed = rms_apply(cand_float, gain_in).astype(jnp.bfloat16).reshape(N_DP * CS, D)
    cand_proj = jnp.dot(cand_normed, weight_in[:, :2 * D], preferred_element_type=jnp.float32)
    cand_gate = jax.nn.silu(cand_proj[:, :D]).astype(jnp.bfloat16)
    cand_query = cand_proj[:, D:].astype(jnp.bfloat16).reshape(N_DP, CS, H, HD)
    block_rows = math.gcd(CS, 1024)
    positions = jnp.arange(LENGTH, dtype=jnp.int32)
    outputs = []
    for dp_index in range(N_DP):
        keys_here = keys[dp_index * HIST_DP:(dp_index + 1) * HIST_DP].astype(jnp.float32)
        values_here = values[dp_index * HIST_DP:(dp_index + 1) * HIST_DP].astype(jnp.float32)
        lengths_here = lengths[dp_index * HIST_DP:(dp_index + 1) * HIST_DP]

        def cross_block(packed):
            query_block, owner = packed
            summed = jnp.zeros((block_rows, H, HD), jnp.float32)
            for member in range(HIST_DP):
                scores = jnp.einsum('che,jhe->chj', query_block.astype(jnp.float32), keys_here[member]) * score_scale
                allowed = (positions[None, None, :] < lengths_here[member]) & (owner[:, None, None] == member)
                weights = jnp.where(allowed, jax.nn.silu(scores), 0.0).astype(jnp.bfloat16)
                summed = summed + jnp.einsum('chj,jhe->che', weights.astype(jnp.float32), values_here[member])
            return summed.astype(jnp.bfloat16)
        blocks = lax.map(cross_block, (cand_query[dp_index].reshape(CS // block_rows, block_rows, H, HD), assignment[dp_index].reshape(CS // block_rows, block_rows)))
        outputs.append(blocks.reshape(CS, D))
    cross_attended = jnp.stack(outputs).reshape(N_DP * CS, D).astype(jnp.float32)
    cand_gated = (rms_apply(cross_attended, gain_attn) * cand_gate.astype(jnp.float32)).astype(jnp.bfloat16)
    candidate_out = (cand_float.reshape(N_DP * CS, D) + jnp.dot(cand_gated, weight_out, preferred_element_type=jnp.float32)).astype(jnp.bfloat16)
    return (history_out, candidate_out.reshape(N_DP, CS, D))
```

```python
import functools

import jax
import jax.numpy as jnp
from jax import lax
from jax.experimental import pallas as pl
from jax.experimental.pallas import tpu as pltpu
from jax.sharding import PartitionSpec as P

H = 16
CAP = 40
ROW_TILE = 16
MESH = pl.DeviceIdType.MESH
F32 = jnp.float32
BF16 = jnp.bfloat16
KEY, VALUE, CAND, QUERY, BACK, CROSS = range(6)


def dot(a, b, dims=((1,), (0,))):
    return lax.dot_general(a, b, (dims, ((), ())), preferred_element_type=F32)


def silu_half(u):
    return u + u * jnp.tanh(u)


def rms_apply(values, gain):
    return values * lax.rsqrt(jnp.mean(values * values, axis=-1, keepdims=True) + 1e-06) * gain


def layer_kernel(
    seq_devices,
    len_ref,
    hist_ref,
    cand_ref,
    owner_ref,
    gain_in_ref,
    gain_attn_ref,
    w_in_ref,
    w_out_ref,
    hist_out_ref,
    cand_out_ref,
    w_buf,
    wo_buf,
    normed_ref,
    gate_ref,
    cand_gate_ref,
    send_kvq,
    send_c,
    recv_k,
    recv_v,
    recv_q,
    recv_c,
    key_heads,
    value_heads,
    att_ref,
    cross_ref,
    back_ref,
    back_c_ref,
    w_sem,
    send_sem,
    recv_sem,
):
    S = seq_devices
    me = lax.axis_index("seq")
    hists, tokens, width = hist_ref.shape
    cands = cand_ref.shape[0]
    heads_here = hists * H // S
    head_dim = width // H
    W = heads_here * head_dim
    blocks = width // W
    window = recv_c.shape[0] // S
    length = tokens * S
    my_hist = me // blocks

    def weight_copy(part):
        return pltpu.make_async_copy(
            w_in_ref.at[:, pl.ds(part * width, width)], w_buf.at[part], w_sem.at[part]
        )

    for part in (2, 3, 1, 0):
        weight_copy(part).start()
    out_copy = pltpu.make_async_copy(w_out_ref, wo_buf, w_sem.at[4])
    out_copy.start()

    barrier = pltpu.get_barrier_semaphore()
    for step in range(1, S):
        pl.semaphore_signal(
            barrier, inc=1, device_id={"seq": lax.rem(me + step, S)}, device_id_type=MESH
        )

    gain_in = gain_in_ref[...]
    hist_rows = hist_ref[...].reshape(hists * tokens, width).astype(F32)
    normed_ref[...] = rms_apply(hist_rows, gain_in).astype(BF16)
    chunk = max(W, min(width, 256))

    def blocks_of(first, value):
        for sub in range(0, chunk, W):
            yield (first + sub) // W, value[:, sub : sub + W]

    def remote(phase, src, dst, other):
        return pltpu.make_async_remote_copy(
            src_ref=src,
            dst_ref=dst,
            send_sem=send_sem.at[phase, other],
            recv_sem=recv_sem.at[phase, me],
            device_id={"seq": other},
            device_id_type=MESH,
        )

    def arrival(phase, ref, rows, source):
        here = ref.at[pl.ds(source * rows, rows), :]
        return pltpu.make_async_remote_copy(
            src_ref=here,
            dst_ref=here,
            send_sem=send_sem.at[phase, source],
            recv_sem=recv_sem.at[phase, source],
            device_id={"seq": source},
            device_id_type=MESH,
        )

    sent = []

    def scatter(phase, src, dst, rows):
        for step in range(1, S):
            other = lax.rem(me + step, S)
            copy = remote(phase, src(other), dst.at[pl.ds(me * rows, rows), :], other)
            copy.start()
            sent.append(copy)

    def project_and_send(phase, part, slot, dst):
        normed = normed_ref[...]
        for first in range(0, width, chunk):
            value = dot(normed, w_buf[part, :, first : first + chunk]).astype(BF16)
            for block, piece in blocks_of(first, value):
                for n in range(hists):
                    send_kvq[slot, n * blocks + block] = piece[n * tokens : (n + 1) * tokens]
        if phase == KEY:
            pl.semaphore_wait(barrier, S - 1)
        scatter(phase, lambda other: send_kvq.at[slot, other], dst, tokens)
        dst[pl.ds(pl.multiple_of(me * tokens, ROW_TILE), tokens), :] = send_kvq[slot, me]

    weight_copy(2).wait()
    project_and_send(KEY, 2, 0, recv_k)
    weight_copy(3).wait()
    project_and_send(VALUE, 3, 1, recv_v)

    cand_rows = cand_ref[...].astype(F32)
    cand_normed = rms_apply(cand_rows, gain_in).astype(BF16)
    owner = owner_ref[...]
    before = (
        lax.broadcasted_iota(jnp.int32, (cands, cands), 0)
        < lax.broadcasted_iota(jnp.int32, (cands, cands), 1)
    ).astype(F32)
    place = jnp.zeros((1, cands), F32)
    for n in range(hists):
        mine = (owner == n).astype(F32)
        rank = dot(jnp.broadcast_to(mine, (8, cands)), before)[0:1]
        place = place + mine * (rank + n * window)
    picks = (
        lax.broadcasted_iota(jnp.int32, (hists * window, cands), 0).astype(F32) == place
    ).astype(F32).astype(BF16)

    weight_copy(1).wait()
    for first in range(0, width, chunk):
        value = dot(cand_normed, w_buf[1, :, first : first + chunk]).astype(BF16)
        value = dot(picks, value).astype(BF16)
        for block, piece in blocks_of(first, value):
            for n in range(hists):
                send_c[n * blocks + block] = piece[n * window : (n + 1) * window]
    scatter(CAND, lambda other: send_c.at[other], recv_c, window)
    recv_c[pl.ds(pl.multiple_of(me * window, ROW_TILE), window), :] = send_c[me]
    project_and_send(QUERY, 1, 2, recv_q)

    weight_copy(0).wait()
    for first in range(0, width, chunk):
        cols = slice(first, first + chunk)
        wide = w_buf[0, :, cols]
        gate_ref[:, cols] = silu_half(0.5 * dot(normed_ref[...], wide)).astype(BF16)
        cand_gate_ref[:, cols] = silu_half(0.5 * dot(cand_normed, wide)).astype(BF16)

    def wait_all(phase, ref, rows):
        for step in range(1, S):
            arrival(phase, ref, rows, lax.rem(me + S - step, S)).wait_recv()

    lane_head = lax.broadcasted_iota(jnp.int32, (1, W), 1) // head_dim
    score_half = 0.5 * head_dim ** (-0.5)
    wait_all(KEY, recv_k, tokens)
    for t in range(heads_here):
        pick = jnp.where(lane_head == t, score_half, 0.0).astype(BF16)
        key_heads[t] = recv_k[...] * pick
    wait_all(VALUE, recv_v, tokens)
    valid = len_ref[my_hist]
    inside = (lax.broadcasted_iota(jnp.int32, (length, W), 0) < valid).astype(F32).astype(BF16)
    values = recv_v[...] * inside
    for t in range(heads_here):
        pick = (lane_head == t).astype(F32).astype(BF16)
        value_heads[t] = values * pick

    key_block = min(length, 256)
    cross_rows = S * window
    cross_step = min(cross_rows, 384)
    wait_all(CAND, recv_c, window)
    for row in range(0, cross_rows, cross_step):
        rows = slice(row, row + cross_step)
        queries = recv_c[rows]
        total = jnp.zeros((cross_step, W), F32)
        for t in range(heads_here):
            for col in range(0, length, key_block):
                cols = slice(col, col + key_block)
                weights = silu_half(dot(queries, key_heads[t, cols], ((1,), (1,))))
                total = total + dot(weights.astype(BF16), value_heads[t, cols])
        cross_ref[rows] = total.astype(BF16)

    def give_back(phase, src, dst, rows, other):
        source = src.at[pl.ds(other * rows, rows), :]

        @pl.when(other != me)
        def _():
            remote(phase, source, dst.at[pl.ds(me * rows, rows), :], other).start()

    for other in range(S):
        give_back(CROSS, cross_ref, back_c_ref, window, other)
    mine = pl.ds(pl.multiple_of(me * window, ROW_TILE), window)
    back_c_ref[mine, :] = cross_ref[mine, :]

    wait_all(QUERY, recv_q, tokens)
    row_ids = lax.broadcasted_iota(jnp.int32, (key_block, key_block), 0)
    col_ids = lax.broadcasted_iota(jnp.int32, (key_block, key_block), 1)
    done = 0
    for row in range(0, length, key_block):
        rows = slice(row, row + key_block)
        queries = recv_q[rows]
        total = jnp.zeros((key_block, W), F32)
        for t in range(heads_here):
            for col in range(0, row + 1, key_block):
                cols = slice(col, col + key_block)
                weights = silu_half(dot(queries, key_heads[t, cols], ((1,), (1,))))
                if col == row:
                    weights = jnp.where(col_ids <= row_ids, weights, 0.0)
                total = total + dot(weights.astype(BF16), value_heads[t, cols])
        att_ref[rows] = total.astype(BF16)
        while (done + 1) * tokens <= row + key_block:
            give_back(BACK, att_ref, back_ref, tokens, done)
            done += 1
    mine = pl.ds(pl.multiple_of(me * tokens, ROW_TILE), tokens)
    back_ref[mine, :] = att_ref[mine, :]

    gain_attn = gain_attn_ref[...]
    out_copy.wait()

    def gather_rows(ref, rows, n):
        parts = [
            ref[(n * blocks + block) * rows : (n * blocks + block + 1) * rows, :]
            for block in range(blocks)
        ]
        return jnp.concatenate(parts, axis=1)

    def project_out(normed, base):
        return (base + dot(normed, wo_buf[...])).astype(BF16)

    wait_all(CROSS, back_c_ref, window)
    windows = jnp.concatenate([gather_rows(back_c_ref, window, n) for n in range(hists)], axis=0)
    cross = dot(picks, windows, ((0,), (0,)))
    cand_gated = (rms_apply(cross, gain_attn) * cand_gate_ref[...].astype(F32)).astype(BF16)
    cand_out_ref[...] = project_out(cand_gated, cand_ref[...].astype(F32))

    wait_all(BACK, back_ref, tokens)
    for n in range(hists):
        attended = gather_rows(back_ref, tokens, n).astype(F32)
        gate = gate_ref[n * tokens : (n + 1) * tokens].astype(F32)
        gated = (rms_apply(attended, gain_attn) * gate).astype(BF16)
        hist_out_ref[n] = project_out(gated, hist_ref[n].astype(F32))

    for copy in sent:
        copy.wait_send()
    for step in range(1, S):
        other = lax.rem(me + step, S)
        for phase, src, dst, rows in (
            (CROSS, cross_ref, back_c_ref, window),
            (BACK, att_ref, back_ref, tokens),
        ):
            source = src.at[pl.ds(other * rows, rows), :]
            remote(phase, source, dst.at[pl.ds(me * rows, rows), :], other).wait_send()


def per_device(history, candidates, lengths, assignment, weight_in, weight_out, gain_in, gain_attn):
    S = lax.axis_size("seq")
    hists, tokens, width = history.shape
    cands = candidates.shape[1]
    heads_here = hists * H // S
    W = heads_here * (width // H)
    length = tokens * S
    window = -(-CAP // ROW_TILE) * ROW_TILE
    rows = hists * tokens
    vmem = pl.BlockSpec(memory_space=pltpu.VMEM)
    smem = pl.BlockSpec(memory_space=pltpu.SMEM)
    hbm = pl.BlockSpec(memory_space=pl.ANY)

    def buf(*shape):
        return pltpu.VMEM(shape, BF16)

    history_out, candidate_out = pl.pallas_call(
        functools.partial(layer_kernel, S),
        out_shape=(
            jax.ShapeDtypeStruct(history.shape, BF16),
            jax.ShapeDtypeStruct((cands, width), BF16),
        ),
        in_specs=[smem, vmem, vmem, vmem, vmem, vmem, hbm, hbm],
        out_specs=(vmem, vmem),
        scratch_shapes=[
            buf(4, width, width),
            buf(width, width),
            buf(rows, width),
            buf(rows, width),
            buf(cands, width),
            buf(3, S, tokens, W),
            buf(S, window, W),
            buf(length, W),
            buf(length, W),
            buf(length, W),
            buf(S * window, W),
            buf(heads_here, length, W),
            buf(heads_here, length, W),
            buf(length, W),
            buf(S * window, W),
            buf(length, W),
            buf(S * window, W),
            pltpu.SemaphoreType.DMA((5,)),
            pltpu.SemaphoreType.DMA((6, S)),
            pltpu.SemaphoreType.DMA((6, S)),
        ],
        compiler_params=pltpu.CompilerParams(
            collective_id=0, has_side_effects=True, vmem_limit_bytes=60 * 1024 * 1024
        ),
        name="gated_layer",
    )(
        lengths,
        history,
        candidates[0],
        assignment,
        gain_in[None],
        gain_attn[None],
        weight_in,
        weight_out,
    )
    return (history_out, candidate_out[None])


def solution(mesh):
    in_specs = (
        P(("groups", "dp"), "seq", None),
        P(("groups", "dp"), "seq", None),
        P(("groups", "dp")),
        P(("groups", "dp"), "seq"),
        P(),
        P(),
        P(),
        P(),
    )
    out_specs = (P(("groups", "dp"), "seq", None), P(("groups", "dp"), "seq", None))
    return jax.shard_map(
        per_device, mesh=mesh, in_specs=in_specs, out_specs=out_specs, check_vma=False
    )
```

```python
import functools

import jax
import jax.numpy as jnp
from jax import lax
from jax.experimental import pallas as pl
from jax.experimental.pallas import tpu as pltpu
from jax.sharding import PartitionSpec as P

H = 16
CAP = 40
ROW_TILE = 16
MESH = pl.DeviceIdType.MESH
F32 = jnp.float32
BF16 = jnp.bfloat16
KEY, VALUE, CAND, QUERY, BACK, CROSS, ROWS = range(7)


def dot(a, b, dims=((1,), (0,))):
    return lax.dot_general(a, b, (dims, ((), ())), preferred_element_type=F32)


def silu_half(u):
    return u + u * jnp.tanh(u)


def rms_apply(values, gain):
    return values * lax.rsqrt(jnp.mean(values * values, axis=-1, keepdims=True) + 1e-06) * gain


def layer_kernel(
    seq_devices,
    len_ref,
    hist_ref,
    cand_ref,
    owner_ref,
    gain_in_ref,
    gain_attn_ref,
    w_in_ref,
    w_out_ref,
    hist_out_ref,
    cand_out_ref,
    w_buf,
    wo_buf,
    normed_ref,
    swap_ref,
    gate_ref,
    cand_gate_ref,
    send_kvq,
    send_c,
    recv_k,
    recv_v,
    recv_q,
    recv_c,
    key_heads,
    value_heads,
    att_ref,
    cross_ref,
    back_ref,
    back_c_ref,
    w_sem,
    send_sem,
    recv_sem,
):
    S = seq_devices
    me = lax.axis_index("seq")
    hists, tokens, width = hist_ref.shape
    cands = cand_ref.shape[0]
    heads_here = hists * H // S
    head_dim = width // H
    W = heads_here * head_dim
    blocks = width // W
    window = recv_c.shape[0] // S
    length = tokens * S
    my_hist = me // blocks
    place_in_half = lax.rem(me, blocks)

    def weight_copy(part):
        return pltpu.make_async_copy(
            w_in_ref.at[:, pl.ds(part * width, width)], w_buf.at[part], w_sem.at[part]
        )

    for part in (2, 3, 1, 0):
        weight_copy(part).start()
    out_copy = pltpu.make_async_copy(w_out_ref, wo_buf, w_sem.at[4])
    out_copy.start()

    barrier = pltpu.get_barrier_semaphore()
    for step in range(1, S):
        pl.semaphore_signal(
            barrier, inc=1, device_id={"seq": lax.rem(me + step, S)}, device_id_type=MESH
        )

    gain_in = gain_in_ref[...]
    hist_rows = hist_ref[...].reshape(hists * tokens, width).astype(F32)
    normed_ref[...] = rms_apply(hist_rows, gain_in).astype(BF16)
    chunk = max(W, min(width, 256))

    def blocks_of(first, value):
        for sub in range(0, chunk, W):
            yield (first + sub) // W, value[:, sub : sub + W]

    def remote(phase, src, dst, other):
        return pltpu.make_async_remote_copy(
            src_ref=src,
            dst_ref=dst,
            send_sem=send_sem.at[phase, other],
            recv_sem=recv_sem.at[phase, me],
            device_id={"seq": other},
            device_id_type=MESH,
        )

    def arrival(phase, ref, rows, source):
        here = ref.at[pl.ds(source * rows, rows), :]
        return pltpu.make_async_remote_copy(
            src_ref=here,
            dst_ref=here,
            send_sem=send_sem.at[phase, source],
            recv_sem=recv_sem.at[phase, source],
            device_id={"seq": source},
            device_id_type=MESH,
        )

    sent = []

    def scatter(phase, src, dst, rows):
        for step in range(1, S):
            other = lax.rem(me + step, S)
            copy = remote(phase, src(other), dst.at[pl.ds(me * rows, rows), :], other)
            copy.start()
            sent.append(copy)

    def swap(step):
        other_hist = lax.rem(my_hist + step, hists)
        return pltpu.make_async_remote_copy(
            src_ref=hist_ref.at[other_hist],
            dst_ref=swap_ref.at[my_hist],
            send_sem=send_sem.at[ROWS, other_hist],
            recv_sem=recv_sem.at[ROWS, my_hist],
            device_id={"seq": other_hist * blocks + place_in_half},
            device_id_type=MESH,
        )

    def project_and_send(phase, part, slot, dst, normed, half):
        for first in range(0, width, chunk):
            value = dot(normed, w_buf[part, :, first : first + chunk]).astype(BF16)
            for block, piece in blocks_of(first, value):
                send_kvq[slot, half * blocks + block] = piece
        shard = half * blocks + place_in_half
        to = dst.at[pl.ds(pl.multiple_of(shard * tokens, ROW_TILE), tokens), :]
        for step in range(1, blocks):
            block = lax.rem(place_in_half + step, blocks)
            copy = pltpu.make_async_remote_copy(
                src_ref=send_kvq.at[slot, half * blocks + block],
                dst_ref=to,
                send_sem=send_sem.at[phase, half * blocks + block],
                recv_sem=recv_sem.at[phase, shard],
                device_id={"seq": my_hist * blocks + block},
                device_id_type=MESH,
            )
            copy.start()
            sent.append(copy)
        to[...] = send_kvq[slot, half * blocks + place_in_half]

    pl.semaphore_wait(barrier, S - 1)
    for step in range(1, hists):
        copy = swap(step)
        copy.start()
        sent.append(copy)

    own = normed_ref[pl.ds(pl.multiple_of(my_hist * tokens, ROW_TILE), tokens), :]
    weight_copy(2).wait()
    project_and_send(KEY, 2, 0, recv_k, own, my_hist)
    weight_copy(3).wait()
    project_and_send(VALUE, 3, 1, recv_v, own, my_hist)

    cand_rows = cand_ref[...].astype(F32)
    cand_normed = rms_apply(cand_rows, gain_in).astype(BF16)
    owner = owner_ref[...]
    before = (
        lax.broadcasted_iota(jnp.int32, (cands, cands), 0)
        < lax.broadcasted_iota(jnp.int32, (cands, cands), 1)
    ).astype(F32)
    place = jnp.zeros((1, cands), F32)
    for n in range(hists):
        mine = (owner == n).astype(F32)
        rank = dot(jnp.broadcast_to(mine, (8, cands)), before)[0:1]
        place = place + mine * (rank + n * window)
    picks = (
        lax.broadcasted_iota(jnp.int32, (hists * window, cands), 0).astype(F32) == place
    ).astype(F32).astype(BF16)

    weight_copy(1).wait()
    for first in range(0, width, chunk):
        value = dot(cand_normed, w_buf[1, :, first : first + chunk]).astype(BF16)
        value = dot(picks, value).astype(BF16)
        for block, piece in blocks_of(first, value):
            for n in range(hists):
                send_c[n * blocks + block] = piece[n * window : (n + 1) * window]
    scatter(CAND, lambda other: send_c.at[other], recv_c, window)
    recv_c[pl.ds(pl.multiple_of(me * window, ROW_TILE), window), :] = send_c[me]
    project_and_send(QUERY, 1, 2, recv_q, own, my_hist)

    weight_copy(0).wait()
    for first in range(0, width, chunk):
        cols = slice(first, first + chunk)
        wide = w_buf[0, :, cols]
        gate_ref[:, cols] = silu_half(0.5 * dot(normed_ref[...], wide)).astype(BF16)
        cand_gate_ref[:, cols] = silu_half(0.5 * dot(cand_normed, wide)).astype(BF16)

    def wait_all(phase, ref, rows):
        for step in range(1, S):
            arrival(phase, ref, rows, lax.rem(me + S - step, S)).wait_recv()

    for step in range(1, hists):
        half = lax.rem(my_hist + step, hists)
        here = swap_ref.at[half]
        pltpu.make_async_remote_copy(
            src_ref=here,
            dst_ref=here,
            send_sem=send_sem.at[ROWS, half],
            recv_sem=recv_sem.at[ROWS, half],
            device_id={"seq": half * blocks + place_in_half},
            device_id_type=MESH,
        ).wait_recv()
        theirs = rms_apply(swap_ref[half].astype(F32), gain_in).astype(BF16)
        project_and_send(KEY, 2, 0, recv_k, theirs, half)
        project_and_send(VALUE, 3, 1, recv_v, theirs, half)
        project_and_send(QUERY, 1, 2, recv_q, theirs, half)

    def wait_shards(phase, ref):
        for turn in range(hists):
            half = lax.rem(my_hist + turn, hists)
            for step in range(1, blocks):
                source = lax.rem(place_in_half + blocks - step, blocks)
                shard = half * blocks + source
                here = ref.at[pl.ds(pl.multiple_of(shard * tokens, ROW_TILE), tokens), :]
                pltpu.make_async_remote_copy(
                    src_ref=here,
                    dst_ref=here,
                    send_sem=send_sem.at[phase, shard],
                    recv_sem=recv_sem.at[phase, shard],
                    device_id={"seq": my_hist * blocks + source},
                    device_id_type=MESH,
                ).wait_recv()

    lane_head = lax.broadcasted_iota(jnp.int32, (1, W), 1) // head_dim
    score_half = 0.5 * head_dim ** (-0.5)
    wait_shards(KEY, recv_k)
    for t in range(heads_here):
        pick = jnp.where(lane_head == t, score_half, 0.0).astype(BF16)
        key_heads[t] = recv_k[...] * pick
    wait_shards(VALUE, recv_v)
    valid = len_ref[my_hist]
    inside = (lax.broadcasted_iota(jnp.int32, (length, W), 0) < valid).astype(F32).astype(BF16)
    values = recv_v[...] * inside
    for t in range(heads_here):
        pick = (lane_head == t).astype(F32).astype(BF16)
        value_heads[t] = values * pick

    key_block = min(length, 256)
    cross_rows = S * window
    cross_step = min(cross_rows, 384)
    wait_all(CAND, recv_c, window)
    for row in range(0, cross_rows, cross_step):
        rows = slice(row, row + cross_step)
        queries = recv_c[rows]
        total = jnp.zeros((cross_step, W), F32)
        for t in range(heads_here):
            for col in range(0, length, key_block):
                cols = slice(col, col + key_block)
                weights = silu_half(dot(queries, key_heads[t, cols], ((1,), (1,))))
                total = total + dot(weights.astype(BF16), value_heads[t, cols])
        cross_ref[rows] = total.astype(BF16)

    def give_back(phase, src, dst, rows, other):
        source = src.at[pl.ds(other * rows, rows), :]

        @pl.when(other != me)
        def _():
            remote(phase, source, dst.at[pl.ds(me * rows, rows), :], other).start()

    for other in range(S):
        give_back(CROSS, cross_ref, back_c_ref, window, other)
    mine = pl.ds(pl.multiple_of(me * window, ROW_TILE), window)
    back_c_ref[mine, :] = cross_ref[mine, :]

    wait_shards(QUERY, recv_q)
    row_ids = lax.broadcasted_iota(jnp.int32, (key_block, key_block), 0)
    col_ids = lax.broadcasted_iota(jnp.int32, (key_block, key_block), 1)
    done = 0
    for row in range(0, length, key_block):
        rows = slice(row, row + key_block)
        queries = recv_q[rows]
        total = jnp.zeros((key_block, W), F32)
        for t in range(heads_here):
            for col in range(0, row + 1, key_block):
                cols = slice(col, col + key_block)
                weights = silu_half(dot(queries, key_heads[t, cols], ((1,), (1,))))
                if col == row:
                    weights = jnp.where(col_ids <= row_ids, weights, 0.0)
                total = total + dot(weights.astype(BF16), value_heads[t, cols])
        att_ref[rows] = total.astype(BF16)
        while (done + 1) * tokens <= row + key_block:
            give_back(BACK, att_ref, back_ref, tokens, done)
            done += 1
    mine = pl.ds(pl.multiple_of(me * tokens, ROW_TILE), tokens)
    back_ref[mine, :] = att_ref[mine, :]

    gain_attn = gain_attn_ref[...]
    out_copy.wait()

    def gather_rows(ref, rows, n):
        parts = [
            ref[(n * blocks + block) * rows : (n * blocks + block + 1) * rows, :]
            for block in range(blocks)
        ]
        return jnp.concatenate(parts, axis=1)

    def project_out(normed, base):
        return (base + dot(normed, wo_buf[...])).astype(BF16)

    wait_all(CROSS, back_c_ref, window)
    windows = jnp.concatenate([gather_rows(back_c_ref, window, n) for n in range(hists)], axis=0)
    cross = dot(picks, windows, ((0,), (0,)))
    cand_gated = (rms_apply(cross, gain_attn) * cand_gate_ref[...].astype(F32)).astype(BF16)
    cand_out_ref[...] = project_out(cand_gated, cand_ref[...].astype(F32))

    wait_all(BACK, back_ref, tokens)
    for n in range(hists):
        attended = gather_rows(back_ref, tokens, n).astype(F32)
        gate = gate_ref[n * tokens : (n + 1) * tokens].astype(F32)
        gated = (rms_apply(attended, gain_attn) * gate).astype(BF16)
        hist_out_ref[n] = project_out(gated, hist_ref[n].astype(F32))

    for copy in sent:
        copy.wait_send()
    for step in range(1, S):
        other = lax.rem(me + step, S)
        for phase, src, dst, rows in (
            (CROSS, cross_ref, back_c_ref, window),
            (BACK, att_ref, back_ref, tokens),
        ):
            source = src.at[pl.ds(other * rows, rows), :]
            remote(phase, source, dst.at[pl.ds(me * rows, rows), :], other).wait_send()


def per_device(history, candidates, lengths, assignment, weight_in, weight_out, gain_in, gain_attn):
    S = lax.axis_size("seq")
    hists, tokens, width = history.shape
    cands = candidates.shape[1]
    heads_here = hists * H // S
    W = heads_here * (width // H)
    length = tokens * S
    window = -(-CAP // ROW_TILE) * ROW_TILE
    rows = hists * tokens
    vmem = pl.BlockSpec(memory_space=pltpu.VMEM)
    smem = pl.BlockSpec(memory_space=pltpu.SMEM)
    hbm = pl.BlockSpec(memory_space=pl.ANY)

    def buf(*shape):
        return pltpu.VMEM(shape, BF16)

    history_out, candidate_out = pl.pallas_call(
        functools.partial(layer_kernel, S),
        out_shape=(
            jax.ShapeDtypeStruct(history.shape, BF16),
            jax.ShapeDtypeStruct((cands, width), BF16),
        ),
        in_specs=[smem, vmem, vmem, vmem, vmem, vmem, hbm, hbm],
        out_specs=(vmem, vmem),
        scratch_shapes=[
            buf(4, width, width),
            buf(width, width),
            buf(rows, width),
            buf(hists, tokens, width),
            buf(rows, width),
            buf(cands, width),
            buf(3, S, tokens, W),
            buf(S, window, W),
            buf(length, W),
            buf(length, W),
            buf(length, W),
            buf(S * window, W),
            buf(heads_here, length, W),
            buf(heads_here, length, W),
            buf(length, W),
            buf(S * window, W),
            buf(length, W),
            buf(S * window, W),
            pltpu.SemaphoreType.DMA((5,)),
            pltpu.SemaphoreType.DMA((7, S)),
            pltpu.SemaphoreType.DMA((7, S)),
        ],
        compiler_params=pltpu.CompilerParams(
            collective_id=0, has_side_effects=True, vmem_limit_bytes=60 * 1024 * 1024
        ),
        name="gated_layer",
    )(
        lengths,
        history,
        candidates[0],
        assignment,
        gain_in[None],
        gain_attn[None],
        weight_in,
        weight_out,
    )
    return (history_out, candidate_out[None])


def solution(mesh):
    in_specs = (
        P(("groups", "dp"), "seq", None),
        P(("groups", "dp"), "seq", None),
        P(("groups", "dp")),
        P(("groups", "dp"), "seq"),
        P(),
        P(),
        P(),
        P(),
    )
    out_specs = (P(("groups", "dp"), "seq", None), P(("groups", "dp"), "seq", None))
    return jax.shard_map(
        per_device, mesh=mesh, in_specs=in_specs, out_specs=out_specs, check_vma=False
    )
```
